32 devices in a mesh: rep: 4 (over z), tp: 8 (over y, x, core).
Axes of the slice: x: 2, y: 2, z: 4, core: 2. Of those that a mesh axis runs over, the one named last changes fastest.
Arguments:
- exp_hidden: bfloat16 [256, 8192], P('rep', 'tp'), may hold values from -160 to 160
- exp_pre_gain: float32 [8192], P('tp'), may hold values from 0.25 to 1.75
- exp_gate: bfloat16 [8192, 28672], P('tp', 'rep'), may hold values from -0.0625 to 0.0625
- exp_up: bfloat16 [8192, 28672], P('tp', 'rep'), may hold values from -0.0625 to 0.0625
- exp_down: bfloat16 [28672, 8192], P('rep', 'tp'), may hold values from -0.03125 to 0.03125
- exp_out_gain: float32 [8192], P('tp'), may hold values from 0.25 to 1.75
- exp_head: bfloat16 [8192, 65536], P(None, ('rep', 'tp')), may hold values from -10 to 10
- ama_hidden: bfloat16 [256, 4096], P('rep', 'tp'), may hold values from -160 to 160
- ama_out_gain: float32 [4096], P('tp'), may hold values from 0.25 to 1.75
- ama_head: bfloat16 [4096, 65536], P(None, ('rep', 'tp')), may hold values from -10 to 10
- logit_scale: float32 [256], replicated, may hold values from 0.25 to 3
- prompt_of: int32 [256], replicated, may hold values from 0 to 7
- prior_picks: int32 [8, 24], replicated, may hold values from 0 to 65535
- valid_mask: int32 [65536], P(('rep', 'tp')), may hold values 0 or 1
Outputs:
- scores: float32 [256, 65536], P(None, ('rep', 'tp'))
- beam_best: float32 [256], replicated
The draws below stay inside these ranges and needn't reach their ends.
All inputs are finite; a program needn't handle non-finite values. No bound on the sum of `valid_mask` on one device may be relied on, other than what follows from the above.
Results may differ from the reference program's by a relative error of at most 0.0034.
Values may be sent and summed in bfloat16 or wider, within the bound.
No kernel may reach another device: no remote copies, remote signals or barrier semaphores. Data moves between devices by JAX's collectives and lax.ppermute only.
A program may use at most 192 MiB of HBM per device.

```python
import jax
import jax.numpy as jnp
from jax import lax

DE = 8192
FFE = 28672
DA = 4096
VOCAB = 65536
PICKS = 24
BEAMS = 256
PROMPTS = 8


favored_count = 16


def favored_entries(key):
    return jax.random.randint(jax.random.fold_in(key, 21), (favored_count,), 0, VOCAB)


def feature_rows(key, rows, width):
    first, second = jax.random.split(key, 2)
    values = jax.random.normal(first, (rows, width), jnp.float32)
    rising = 0.6 + 1.2 * jnp.arange(width, dtype=jnp.float32) / width
    rough = jnp.exp(jax.random.uniform(second, (width,), jnp.float32, -0.35, 0.35))
    values = values * rising[None, :] * rough[None, :]
    return jnp.clip(values, -160.0, 160.0).astype(jnp.bfloat16)


def head_columns(base_key, key, width, entries):
    first = jax.random.fold_in(key, 0)
    second = jax.random.fold_in(key, 1)
    fifth = jax.random.fold_in(key, 4)
    values = jax.random.normal(first, (width, entries), jnp.float32) / jnp.sqrt(width * 1.0)
    rising = 1.0 + jnp.arange(entries, dtype=jnp.float32) / entries
    rough = jnp.exp(jax.random.uniform(second, (entries,), jnp.float32, -0.3, 0.3))
    column_scale = rising * rough
    favored = favored_entries(base_key)
    entry_ids = jnp.arange(entries, dtype=jnp.int32)
    is_favored = jnp.any(entry_ids[:, None] == favored[None, :], axis=1)
    lift = jnp.exp(jax.random.uniform(fifth, (entries,), jnp.float32, 1.4, 1.8))
    column_scale = jnp.where(is_favored, lift * rising * rough, column_scale)
    return jnp.clip(values * column_scale[None, :], -10.0, 10.0).astype(jnp.bfloat16)


def draw_exp_hidden(key, part):
    return feature_rows(jax.random.fold_in(key, 11), BEAMS, DE)


def draw_ama_hidden(key, part):
    return feature_rows(jax.random.fold_in(key, 12), BEAMS, DA)


def draw_exp_head(key, part):
    return head_columns(key, jax.random.fold_in(key, 13), DE, VOCAB)


def draw_ama_head(key, part):
    return head_columns(key, jax.random.fold_in(key, 14), DA, VOCAB)


def draw_logit_scale(key, part):
    inner = jax.random.fold_in(key, 15)
    return jnp.exp(jax.random.uniform(inner, (BEAMS,), jnp.float32, -0.693, 0.693))


def draw_prior_picks(key, part):
    favored = favored_entries(key)
    first, second, third = jax.random.split(jax.random.fold_in(key, 22), 3)
    which = jax.random.randint(first, (PROMPTS, PICKS), 0, favored_count)
    from_favored = jnp.take(favored, which)
    anywhere = jax.random.randint(second, (PROMPTS, PICKS), 0, VOCAB)
    coin = jax.random.randint(third, (PROMPTS, PICKS), 0, 4)
    return jnp.where(coin < 3, from_favored, anywhere).astype(jnp.int32)


def with_ends(array, rng, low, high):
    index_at = [jax.random.randint(jax.random.fold_in(rng, axis), (), 0, length) for axis, length in enumerate(array.shape)]
    widest = array.shape.index(max(array.shape))
    next_to = index_at[:widest] + [(index_at[widest] + 1) % array.shape[widest]] + index_at[widest + 1:]
    return array.at[tuple(index_at)].set(low).at[tuple(next_to)].set(high)


def levels(key, dims, cuts, smallest, top_value):
    def one(axis_at, shards_of):
        draws = jax.random.uniform(jax.random.fold_in(jax.random.fold_in(key, 6), axis_at), (shards_of,), jnp.float32, smallest / len(cuts), top_value / len(cuts))
        return jnp.repeat(jnp.exp(draws), dims[axis_at] // shards_of).reshape((-1,) + (1,) * (len(dims) - axis_at - 1))

    level = one(*cuts[0])
    for cut in cuts[1:]:
        level = level * one(*cut)
    return level


def bell_draw(stream_key, dims, scale, reach, cuts=(), kind=jnp.bfloat16):
    values = scale * jax.random.normal(stream_key, dims, jnp.float32)
    if cuts:
        values = values * levels(stream_key, dims, cuts, -0.22, 0.18)
    return jnp.clip(values, -reach, reach).astype(kind)


def setup_inputs(seed: int = 0) -> dict:
    keys = jax.random.split(jax.random.key(seed), 15)
    exp_hidden = draw_exp_hidden(jax.random.fold_in(keys[14], 71), 0)
    exp_pre_gain = jnp.clip(1.0 + 0.15 * jax.random.normal(keys[1], (DE,), jnp.float32), 0.25, 1.75)
    exp_gate = bell_draw(keys[2], (DE, FFE), DE ** -0.5, 0.0625, ((0, 8), (1, 4)))
    exp_up = bell_draw(keys[3], (DE, FFE), DE ** -0.5, 0.0625, ((0, 8), (1, 4)))
    exp_down = bell_draw(keys[4], (FFE, DE), FFE ** -0.5, 0.03125, ((0, 4), (1, 8)))
    exp_out_gain = jnp.clip(1.0 + 0.15 * jax.random.normal(keys[5], (DE,), jnp.float32), 0.25, 1.75)
    exp_head = draw_exp_head(jax.random.fold_in(keys[14], 71), 0)
    ama_hidden = draw_ama_hidden(jax.random.fold_in(keys[14], 71), 0)
    ama_out_gain = jnp.clip(1.0 + 0.15 * jax.random.normal(keys[8], (DA,), jnp.float32), 0.25, 1.75)
    ama_head = draw_ama_head(jax.random.fold_in(keys[14], 71), 0)
    logit_scale = draw_logit_scale(jax.random.fold_in(keys[14], 71), 0)
    prompt_of = with_ends(jax.random.randint(keys[11], (BEAMS,), 0, PROMPTS), jax.random.fold_in(keys[11], 1), 0, PROMPTS - 1).astype(jnp.int32)
    prior_picks = draw_prior_picks(jax.random.fold_in(keys[14], 71), 0)
    valid_mask = with_ends((jax.random.randint(keys[13], (VOCAB,), 0, 8) < 7).astype(jnp.int32), jax.random.fold_in(keys[13], 1), 0, 1)
    return dict(exp_hidden=exp_hidden, exp_pre_gain=exp_pre_gain, exp_gate=exp_gate, exp_up=exp_up, exp_down=exp_down, exp_out_gain=exp_out_gain, exp_head=exp_head, ama_hidden=ama_hidden, ama_out_gain=ama_out_gain, ama_head=ama_head, logit_scale=logit_scale, prompt_of=prompt_of, prior_picks=prior_picks, valid_mask=valid_mask)


norm_epsilon = 1e-05
contrast_weight = 0.5
hamming_weight = 0.7

def normed_rows(values, gain):
    meansq = lax.optimization_barrier(jnp.mean(values * values, axis=1, keepdims=True))
    return (values * lax.rsqrt(meansq + norm_epsilon) * gain).astype(jnp.bfloat16)

def head_logp(final, head, logit_scale):
    logits = logit_scale[:, None] * jnp.dot(final, head, preferred_element_type=jnp.float32)
    largest = lax.optimization_barrier(jnp.max(logits, axis=1, keepdims=True))
    totals = lax.optimization_barrier(jnp.sum(jnp.exp(logits - largest), axis=1, keepdims=True))
    return logits - largest - jnp.log(totals)

def reference(exp_hidden, exp_pre_gain, exp_gate, exp_up, exp_down, exp_out_gain, exp_head, ama_hidden, ama_out_gain, ama_head, logit_scale, prompt_of, prior_picks, valid_mask):
    values = exp_hidden.astype(jnp.float32)
    normed = normed_rows(values, exp_pre_gain)
    gate = jnp.dot(normed, exp_gate, preferred_element_type=jnp.float32)
    up = jnp.dot(normed, exp_up, preferred_element_type=jnp.float32)
    hidden = (jax.nn.silu(gate) * up).astype(jnp.bfloat16)
    layer = values + jnp.dot(hidden, exp_down, preferred_element_type=jnp.float32)
    final_exp = normed_rows(layer, exp_out_gain)
    final_ama = normed_rows(ama_hidden.astype(jnp.float32), ama_out_gain)
    logp_exp = head_logp(final_exp, exp_head, logit_scale)
    logp_ama = head_logp(final_ama, ama_head, logit_scale)
    picks_row = jnp.take(prior_picks, prompt_of, axis=0)
    vocab_ids = jnp.arange(VOCAB, dtype=jnp.int32)

    def add_pick(index, counts):
        column = lax.dynamic_slice_in_dim(picks_row, index, 1, 1)
        return counts + (column == vocab_ids[None, :]).astype(jnp.float32)
    counts = lax.fori_loop(0, PICKS, add_pick, jnp.zeros((BEAMS, VOCAB), jnp.float32))
    valid = valid_mask.astype(jnp.float32)[None, :]
    scores = logp_exp - contrast_weight * valid * logp_ama - hamming_weight * counts
    return (scores, lax.optimization_barrier(jnp.max(scores, axis=1)))
```

```python
import jax
import jax.numpy as jnp
import numpy as np
from jax import lax
from jax.sharding import PartitionSpec as P


norm_epsilon = 1e-05
contrast_weight = 0.5
hamming_weight = 0.7
chunk_count = 4

bf16 = jnp.bfloat16
f32 = jnp.float32


def bits_of(size):
    return [1 << k for k in range(size.bit_length() - 1)]


def tree(values, combine):
    values = list(values)
    while len(values) > 1:
        values = [combine(values[k], values[k + 1]) for k in range(0, len(values), 2)]
    return values[0]


def merged(stats):
    tops = tree([s[0::2][:2] for s in stats], jnp.maximum)
    totals = tree([s[1::2][:2] * jnp.exp(s[0::2][:2] - tops) for s in stats], jnp.add)
    bests = tree([s[4:6] for s in stats], jnp.maximum)
    return jnp.stack([tops[0], totals[0], tops[1], totals[1], bests[0], bests[1]])


def make_body(tp_size, rep_size):
    tp_bits, rep_bits = bits_of(tp_size), bits_of(rep_size)
    near, far = tp_bits[:1], tp_bits[1:]
    blocks = max(tp_size, rep_size)
    tp_step, rep_step = blocks // tp_size, blocks // rep_size

    def over_tp(value, bit):
        return lax.ppermute(value, "tp", [(k, k ^ bit) for k in range(tp_size)])

    def over_rep(value, bit):
        return lax.ppermute(value, "rep", [(k, k ^ bit) for k in range(rep_size)])

    def tp_sum(value):
        for bit in tp_bits:
            value = value + over_tp(value, bit)
        return value

    block_bits = bits_of(blocks)

    def order_of(first_bits):
        first = [bit * tp_step for bit in first_bits]
        return first + [bit for bit in block_bits if bit not in first]

    def positions(order):
        count = len(order)
        return np.array(
            [
                sum(bit for k, bit in enumerate(order) if q >> (count - 1 - k) & 1)
                for q in range(blocks)
            ],
            np.int32,
        )

    colors = [near + far, near + far[::-1]]
    orders = [order_of(color) for color in colors]

    def body(
        exp_hidden,
        exp_pre_gain,
        exp_gate,
        exp_up,
        exp_down,
        exp_out_gain,
        exp_head,
        ama_hidden,
        ama_out_gain,
        ama_head,
        logit_scale,
        prompt_of,
        prior_picks,
        valid_mask,
    ):
        rep_rows, width = exp_hidden.shape
        rows = rep_rows * rep_size
        block_rows = rows // blocks
        full_width = width * tp_size
        ama_width = ama_hidden.shape[1]
        full_ama_width = ama_width * tp_size
        here, plane = lax.axis_index("tp"), lax.axis_index("rep")
        offset = (here * tp_step) ^ (plane * rep_step)
        every_row = jnp.arange(rows, dtype=jnp.int32)

        def actual_rows(order):
            at = jnp.asarray(positions(order)) ^ offset
            return (at[:, None] * block_rows + jnp.arange(block_rows, dtype=jnp.int32)).reshape(-1)

        def relative_to_rep(actual):
            return ((actual // rep_rows) ^ plane) * rep_rows + actual % rep_rows

        def gathered_rep(value):
            return jnp.concatenate([value] + [over_rep(value, k) for k in range(1, rep_size)], 0)

        rows_rel = gathered_rep(exp_hidden)
        actual = [actual_rows(order) for order in orders]
        source = relative_to_rep(jnp.concatenate(actual))
        picks = (source[:, None] == every_row[None, :]).astype(bf16)
        ordered = jnp.dot(picks, rows_rel, preferred_element_type=f32)
        gained = (ordered * exp_pre_gain[None, :]).astype(bf16)
        color_rows = [gained[:rows], gained[rows:]]

        values_ama = ama_hidden.astype(f32)
        ama_rows = (values_ama * ama_out_gain[None, :]).astype(bf16)
        ama_squares = jnp.sum(values_ama * values_ama, axis=1)
        values_rel = rows_rel.astype(f32)
        squares = tp_sum(
            jnp.stack([jnp.sum(values_rel * values_rel, axis=1), gathered_rep(ama_squares)])
        )
        factors = lax.rsqrt(
            squares / jnp.array([[full_width], [full_ama_width]], f32) + norm_epsilon
        )
        own_count = rows // tp_size
        own_at = relative_to_rep(actual[0][:own_count])
        own_factor = jnp.sum(
            jnp.where(own_at[:, None] == every_row[None, :], factors[0][None, :], 0.0), axis=1
        )

        def gathered_blocks(value, bits):
            held = [(0, value)]
            for bit in bits:
                held = held + [(at ^ bit, over_tp(v, bit)) for at, v in held]
            return held

        ama_held = gathered_blocks(ama_rows, far)
        ama_wide = jnp.concatenate([v for _, v in ama_held], axis=1)
        ama_wide, _ = lax.optimization_barrier((ama_wide, rows_rel))
        ama_wide = gathered_rep(ama_wide)
        from_rep = relative_to_rep(every_row)
        ama_picks = (from_rep[:, None] == every_row[None, :]).astype(bf16)
        ama_wide = jnp.dot(ama_picks, ama_wide, preferred_element_type=f32).astype(bf16)
        ama_sides = gathered_blocks(ama_wide, near)
        full_ama = jnp.zeros((rows, full_ama_width), bf16)
        for side, wide in ama_sides:
            for k, (at, _) in enumerate(ama_held):
                full_ama = lax.dynamic_update_slice(
                    full_ama,
                    wide[:, k * ama_width : (k + 1) * ama_width],
                    (0, (here ^ at ^ side) * ama_width),
                )
        ama_factor = jnp.sum(
            jnp.where(from_rep[:, None] == every_row[None, :], factors[1][None, :], 0.0), axis=1
        )
        raw_ama = jnp.dot(full_ama, ama_head, preferred_element_type=f32)

        hidden_width = exp_gate.shape[1]
        chunk = hidden_width // chunk_count
        terms = [None, None]
        for c in range(chunk_count):
            color = c % 2
            lo, hi = c * chunk, (c + 1) * chunk
            both = jnp.concatenate(
                [
                    jnp.dot(color_rows[color], exp_gate[:, lo:hi], preferred_element_type=f32),
                    jnp.dot(color_rows[color], exp_up[:, lo:hi], preferred_element_type=f32),
                ],
                axis=1,
            )
            for bit in colors[color]:
                half = both.shape[0] // 2
                both = both[:half] + over_tp(both[half:].astype(bf16), bit).astype(f32)
            gate = both[:, :chunk] * own_factor[:, None]
            up = both[:, chunk:] * own_factor[:, None]
            hidden = (jax.nn.silu(gate) * up).astype(bf16)
            for bit in colors[color][::-1]:
                hidden = jnp.concatenate([hidden, over_tp(hidden, bit)], axis=0)
            term = jnp.dot(hidden, exp_down[lo:hi], preferred_element_type=f32)
            terms[color] = term if terms[color] is None else terms[color] + term

        cube = (2,) * len(block_bits)
        total = terms[0].reshape(cube + (block_rows, width))
        if terms[1] is not None:
            second = terms[1].reshape(cube + (block_rows, width))
            axes = [orders[1].index(bit) for bit in orders[0]] + [len(cube), len(cube) + 1]
            total = total + second.transpose(axes)

        values = ordered[:rows].reshape(cube + (block_rows, width))
        left = list(orders[0])
        stages = []
        for bit in rep_bits:
            axis = left.index(bit * rep_step)
            send = lax.index_in_dim(total, 1, axis, keepdims=False).astype(bf16)
            total = lax.index_in_dim(total, 0, axis, keepdims=False) + over_rep(send, bit).astype(f32)
            values = lax.index_in_dim(values, 0, axis, keepdims=False)
            left.pop(axis)
            stages.append((axis, bit))
        layer = values + total
        layer_squares = jnp.sum(layer * layer, axis=-1)
        final = (layer * exp_out_gain).astype(bf16)
        for axis, bit in stages[::-1]:
            final = jnp.stack([final, over_rep(final, bit)], axis)
            layer_squares = jnp.stack([layer_squares, over_rep(layer_squares, bit)], axis)
        back = actual[0][None, :] == every_row[:, None]
        final = jnp.dot(
            back.astype(bf16), final.reshape(rows, width), preferred_element_type=f32
        ).astype(bf16)
        layer_squares = jnp.sum(jnp.where(back, layer_squares.reshape(1, rows), 0.0), axis=1)
        exp_factor = lax.rsqrt(tp_sum(layer_squares) / full_width + norm_epsilon)

        half = rows // 2
        full_exp = jnp.zeros((rows, full_width), bf16)
        for part in range(2):
            piece = final[part * half : (part + 1) * half]
            for at, value in gathered_blocks(piece, colors[part][1:] + near):
                full_exp = lax.dynamic_update_slice(
                    full_exp, value, (part * half, (here ^ at) * width)
                )
        raw_exp = jnp.dot(full_exp, exp_head, preferred_element_type=f32)

        logits_exp = (logit_scale * exp_factor)[:, None] * raw_exp
        logits_ama = (logit_scale * ama_factor)[:, None] * raw_ama

        entries = exp_head.shape[1]
        first_entry = lax.axis_index(("rep", "tp")) * entries
        vocab_ids = first_entry + jnp.arange(entries, dtype=jnp.int32)
        prompts = prior_picks.shape[0]
        prompt_counts = jnp.sum(
            (prior_picks[:, :, None] == vocab_ids[None, None, :]).astype(f32), axis=1
        )
        of_prompt = prompt_of[:, None] == jnp.arange(prompts, dtype=jnp.int32)[None, :]
        counts = jnp.dot(
            of_prompt.astype(bf16), prompt_counts.astype(bf16), preferred_element_type=f32
        )
        valid = valid_mask[None, :] != 0
        penalty = hamming_weight * counts

        top_exp, top_ama = jnp.max(logits_exp, axis=1), jnp.max(logits_ama, axis=1)
        total_exp = jnp.sum(jnp.exp(logits_exp - top_exp[:, None]), axis=1)
        total_ama = jnp.sum(jnp.exp(logits_ama - top_ama[:, None]), axis=1)
        plain = logits_exp - penalty
        lowered = plain - contrast_weight * logits_ama
        best_valid = jnp.max(jnp.where(valid, lowered, -jnp.inf), axis=1)
        best_other = jnp.max(jnp.where(valid, -jnp.inf, plain), axis=1)
        stats = jnp.stack([top_exp, total_exp, top_ama, total_ama, best_valid, best_other])
        stats = merged([stats] + [over_tp(stats, k) for k in range(1, tp_size)])
        stats = merged([stats] + [over_rep(stats, k) for k in range(1, rep_size)])
        norm_exp = stats[0] + jnp.log(stats[1])
        norm_ama = stats[2] + jnp.log(stats[3])
        scores = jnp.where(
            valid, lowered + (contrast_weight * norm_ama)[:, None], plain
        ) - norm_exp[:, None]
        beam_best = jnp.maximum(stats[4] + contrast_weight * norm_ama, stats[5]) - norm_exp
        return (scores, beam_best)

    return body


def solution(mesh):
    placed = (
        P("rep", "tp"),
        P("tp"),
        P("tp", "rep"),
        P("tp", "rep"),
        P("rep", "tp"),
        P("tp"),
        P(None, ("rep", "tp")),
        P("rep", "tp"),
        P("tp"),
        P(None, ("rep", "tp")),
        P(),
        P(),
        P(),
        P(("rep", "tp")),
    )
    return jax.shard_map(
        make_body(mesh.shape["tp"], mesh.shape["rep"]),
        mesh=mesh,
        in_specs=placed,
        out_specs=(P(None, ("rep", "tp")), P()),
        check_vma=False,
    )
```
